256 devices in a mesh: swath: 8 (over y_hi, x), bulk: 32 (over y_lo, z, core).
Axes of the slice: x: 4, y: 4 (y_hi: 2, y_lo: 2; y = y_hi * 2 + y_lo), z: 8, core: 2. Of those that a mesh axis runs over, the one named last changes fastest.
Arguments:
- image: float32 [32, 2048, 1024], P('bulk', None, 'swath'), may hold values from -6 to 6
- offsets: int32 [32], P('bulk'), may hold values from -128 to 127
Outputs:
- defect: float32 [32, 2048, 1024], P('bulk', None, 'swath')
The draws below stay inside these ranges and needn't reach their ends.
All inputs are finite; a program needn't handle non-finite values.
Results may differ from the reference program's by a relative error of at most 0.00025.
Values sent between devices are 32-bit elements; how exact they have to be, the bound alone decides.
No kernel may reach another device: no remote copies, remote signals or barrier semaphores. Data moves between devices by JAX's collectives and lax.ppermute only.
A program may use at most 64 MiB of HBM per device.

```python
import math
import jax
import jax.numpy as jnp
from jax import lax

COLS = 2048
TPD = 1
DIE_SPAN = 4
TILES = 32
HEIGHT = 1024


def with_ends(array, rng, smallest, top_value):
    spot = [jax.random.randint(jax.random.fold_in(rng, axis), (), 0, length) for axis, length in enumerate(array.shape)]
    widest = array.shape.index(max(array.shape))
    next_to = spot[:widest] + [(spot[widest] + 1) % array.shape[widest]] + spot[widest + 1:]
    return array.at[tuple(spot)].set(smallest).at[tuple(next_to)].set(top_value)


def levels(rng, shape, pieces, least, top_value):
    level, own = 1.0, jax.random.fold_in(rng, 6)
    for axis_at, parts in pieces:
        heights = jnp.exp(jax.random.uniform(jax.random.fold_in(own, axis_at), (parts,), jnp.float32, least / len(pieces), top_value / len(pieces)))
        level = level * jnp.repeat(heights, shape[axis_at] // parts).reshape([-1 if axis == axis_at else 1 for axis in range(len(shape))])
    return level


def centred(own_key, dims, spread, limit, pieces=(), kind=jnp.bfloat16):
    gain = levels(own_key, dims, pieces, -0.22, 0.18) if pieces else 1.0
    drawn = jax.random.normal(own_key, dims, jnp.float32) * spread * gain
    return jnp.minimum(jnp.maximum(drawn, -limit), limit).astype(kind)


def setup_inputs(seed: int = 0) -> dict:
    arg_keys = jax.random.split(jax.random.key(seed), 3)
    return {
        "image": centred(arg_keys[0], (TILES, COLS, HEIGHT), 1.0, 6.0, ((0, 32), (2, 8)), jnp.float32),
        "offsets": with_ends(jax.random.randint(arg_keys[1], (TILES,), -128, 128), jax.random.fold_in(arg_keys[1], 1), -128, 127).astype(jnp.int32),
    }


GAINS = (1.0, 2.0, 4.0, 8.0)
TAPS = (0.0625, 0.25, 0.375, 0.25, 0.0625)


def shift_tile(picture, offset):
    col_count = picture.shape[0]
    indices = jnp.arange(col_count, dtype=jnp.int32)
    signed = jnp.where(indices < col_count // 2, indices, indices - col_count).astype(jnp.float32)
    angles = signed * offset.astype(jnp.float32) * (-2.0 * math.pi / (64.0 * col_count))
    spectrum = jnp.fft.fft(picture, axis=0)
    turned = spectrum * (jnp.cos(angles) + 1j * jnp.sin(angles))[:, None]
    return jnp.real(jnp.fft.ifft(turned, axis=0)).astype(picture.dtype)


def blur(values, dimension, spacing):
    length = values.shape[dimension]
    widths = [(0, 0), (0, 0)]
    widths[dimension] = (2 * spacing, 2 * spacing)
    padded = jnp.pad(values, widths)
    result = jnp.zeros_like(values)
    for position, weight in enumerate(TAPS):
        result = result + weight * lax.slice_in_dim(padded, position * spacing, position * spacing + length, axis=dimension)
    return result


def score_tile(picture):
    current = picture
    result = jnp.zeros_like(picture)
    for octave in range(4):
        spacing = 2 ** octave
        coarser = blur(blur(current, 0, spacing), 1, spacing)
        result = result + GAINS[octave] * (current - coarser) ** 2
        current = coarser
    return result


def reference(image, offsets):
    partner = TPD * DIE_SPAN
    tile_total = image.shape[0]
    moved = lax.map(lambda packed: shift_tile(packed[0], packed[1]), (image[:tile_total - partner], offsets[:tile_total - partner]))
    ahead_part = moved - image[partner:]
    behind_part = -lax.map(lambda packed: shift_tile(packed[0], -packed[1]), (ahead_part, offsets[:tile_total - partner]))
    ahead = jnp.concatenate([ahead_part, behind_part[tile_total - 2 * partner:]], axis=0)
    behind = jnp.concatenate([ahead_part[:partner], behind_part], axis=0)
    return lax.map(lambda packed: score_tile(packed[0]) * score_tile(packed[1]), (ahead, behind))
```

```python
import functools
import math

import jax
import jax.numpy as jnp
from jax import lax
from jax.experimental import pallas as pl
from jax.experimental.pallas import tpu as pltpu
from jax.sharding import PartitionSpec as P

DIE_SPAN = 4
COLS = 2048
LANES = 128
HALO = 32
ROWS_A = 1344
ROWS_B = COLS - ROWS_A
KEEP_A = ROWS_A - 32
WINDOW = 192
WINDOWS_A = -(-KEEP_A // WINDOW)
WINDOWS_B = -(-(COLS - KEEP_A) // WINDOW)
START_B = COLS - WINDOWS_B * WINDOW - HALO
OLD_B = ROWS_A - START_B

F32 = jnp.float32
BF16 = jnp.bfloat16
VMEM = pl.BlockSpec(memory_space=pltpu.VMEM)
SMEM = pl.BlockSpec(memory_space=pltpu.SMEM)
ANY = pl.BlockSpec(memory_space=pl.ANY)
PARAMS = pltpu.CompilerParams(vmem_limit_bytes=40 << 20)


def split(value):
    high = value.astype(BF16)
    return high, (value - high.astype(F32)).astype(BF16)


def tables_kernel(flags, row_high, row_low, col_high, col_low):
    shape = (256, 256)
    down = lax.broadcasted_iota(jnp.int32, shape, 0)
    across = lax.broadcasted_iota(jnp.int32, shape, 1)
    apart = (down - across) & 255
    apart = jnp.minimum(apart, 256 - apart)
    blurs = []
    for octave in range(4):
        reach = 2**octave
        weight = jnp.where(apart == 0, 6.0, jnp.where(apart == reach, 4.0, jnp.where(apart == 2 * reach, 1.0, 0.0)))
        blurs.append(weight.astype(BF16))
    inside = (across < LANES).astype(jnp.int32)
    inside = inside + ((across >= LANES) & (across < LANES + HALO)).astype(jnp.int32) * flags[3]
    inside = (inside + (across >= 256 - HALO).astype(jnp.int32) * flags[2]).astype(F32)
    total = jnp.where(down == across, inside, 0.0)
    for octave in range(4):
        high, low = split(total)
        total = inside * (
            jnp.dot(high, blurs[octave], preferred_element_type=F32)
            + jnp.dot(low, blurs[octave], preferred_element_type=F32)
        )
        high, low = split(total[:, :LANES] * 256.0 ** -(octave + 1))
        row_high[:, octave * LANES : (octave + 1) * LANES] = high
        if octave >= 2:
            row_low[:, (octave - 2) * LANES : (octave - 1) * LANES] = low
    for case, inside in enumerate((down >= HALO, down >= 0, down < 256 - HALO)):
        inside = inside.astype(F32)
        total = jnp.where(down == across, inside, 0.0)
        for octave in range(4):
            high, low = split(total)
            total = inside * (
                jnp.dot(blurs[octave], high, preferred_element_type=F32)
                + jnp.dot(blurs[octave], low, preferred_element_type=F32)
            )
            high, low = split(total[HALO : 256 - HALO])
            col_high[case, octave] = high
            if octave >= 2:
                col_low[case, octave - 2] = low


def lanes(shape):
    return lax.broadcasted_iota(jnp.int32, shape, 1)


def signs(shape):
    return (1 - 2 * (lax.broadcasted_iota(jnp.int32, shape, 0) % 2)).astype(F32)


def sine(x):
    y = x * x
    total = jnp.full_like(x, 1 / math.factorial(13))
    for power in (11, 9, 7, 5, 3, 1):
        total = total * y + (-1) ** ((power - 1) // 2) / math.factorial(power)
    return total * x


def cosine(x):
    y = x * x
    total = jnp.full_like(x, -1 / math.factorial(14))
    for power in (12, 10, 8, 6, 4, 2, 0):
        total = total * y + (-1) ** (power // 2) / math.factorial(power)
    return total


def turned_sine(moves):
    turns = jnp.floor(moves * (1 / 64) + 0.5)
    parity = turns - 2 * jnp.floor(turns * 0.5)
    return (1 - 2 * parity) * sine((moves - 64 * turns) * (math.pi / 64))


def nyquist(v):
    folded = v.reshape(COLS // 8, 8, LANES).sum(axis=0)
    return jnp.sum(folded * signs((8, LANES)), axis=0, keepdims=True) * (1 / COLS)


def pack(v, out_left, out_right, at):
    n = v.shape[0] // 4
    lane = lanes((n, LANES))
    left = right = None
    for q in range(4):
        piece = v[q * n : (q + 1) * n]
        here = (lane >= 32 * q) & (lane < 32 * q + 32)
        to_left = pltpu.roll(piece, 32 * q, 1) if q else piece
        to_right = pltpu.roll(piece, (32 * q + 32) % 128, 1) if q < 3 else piece
        left = to_left if left is None else jnp.where(here, to_left, left)
        right = to_right if right is None else jnp.where(here, to_right, right)
    out_left[at : at + n, :] = left
    out_right[at : at + n, :] = right


def unpack(from_right, from_left, q):
    lane = lanes(from_right.shape)
    right = pltpu.roll(from_right, (128 - 32 * q) % 128, 1) if q else from_right
    left = pltpu.roll(from_left, (96 - 32 * q) % 128, 1) if q < 3 else from_left
    return jnp.where(lane < HALO, right, jnp.where(lane >= LANES - HALO, left, 0.0))


def head_kernel(move, x, adn, aup, ny, pleft, pright):
    v = x[...]
    own = move[0].astype(F32)
    tone = nyquist(v)
    ny[...] = jnp.broadcast_to(tone, (8, LANES))
    wave = turned_sine(jnp.full((8, LANES), own, F32))
    swing = (wave * wave * jnp.broadcast_to(tone, (8, LANES)) * signs((8, LANES)))[None]
    adn[...] = v[:ROWS_A]
    first = v[:ROWS_A].reshape(ROWS_A // 8, 8, LANES) - swing
    aup[:ROWS_A, :] = first.reshape(ROWS_A, LANES)
    aup[ROWS_A:, :] = jnp.full((8, LANES), own, F32)
    pack(v, pleft, pright, 0)


def edge_kernel(move, x, ny, from_right, from_left, h, bdn, bup):
    n = COLS // 4
    for q in range(4):
        h[q * n : (q + 1) * n, :] = unpack(from_right[...], from_left[...], q)
    own = move[0].astype(F32)
    wave = turned_sine(jnp.full((8, LANES), own, F32))
    gain = wave * wave * signs((8, LANES))
    swing = (gain * ny[...])[None]
    hswing = (gain * jnp.broadcast_to(nyquist(h[...]), (8, LANES)))[None]
    half = ROWS_B // 2
    lane = lanes((half, LANES))

    def put(main, edge, out):
        out[:ROWS_B, :] = main
        one, two = edge[:half], edge[half:]
        out[ROWS_B:, :] = jnp.where(
            lane < 32,
            one,
            jnp.where(lane < 64, pltpu.roll(two, 32, 1), jnp.where(lane < 96, pltpu.roll(one, 96, 1), two)),
        )

    main = x[ROWS_A:, :]
    edge = h[ROWS_A:, :]
    put(main, edge, bdn)
    shape = (ROWS_B // 8, 8, LANES)
    put(
        (main.reshape(shape) - swing).reshape(ROWS_B, LANES),
        (edge.reshape(shape) - hswing).reshape(ROWS_B, LANES),
        bup,
    )


def shift_kernel(sign, move, x, h, out, hi, lo, ev, od):
    if sign > 0:
        moves = jnp.full((8, COLS), move[0].astype(F32), F32)
    else:
        moves = -jnp.concatenate([move[ROWS_A:, :]] * (COLS // LANES), axis=1)
    place = lax.broadcasted_iota(jnp.int32, (8, COLS), 1)
    delay = (1024 - place).astype(F32)
    steps = 64 * delay - moves
    turns = jnp.floor(steps * (1 / 65536) + 0.5)
    rest = steps - 65536 * turns
    flip = 1 - 2 * (turns - 2 * jnp.floor(turns * 0.5))
    theta = rest * (math.pi / 65536)
    hit = rest == 0.0
    parity = (1 - 2 * (place % 2)).astype(F32)
    base = parity * turned_sine(moves) * (-0.5 / 1024) / jnp.where(hit, 1.0, sine(theta))
    even = jnp.where(hit, 0.5, base * cosine(theta))
    odd = flip * jnp.where(hit, 0.5, base)
    for part, row in enumerate((even, odd)):
        slope = pltpu.roll(row, 0, 1, stride=1, stride_axis=0)
        for g in range(32):
            band = pltpu.roll(slope, 8 * g, 1) if g else slope
            top = band.astype(BF16)
            hi[part, 8 * g : 8 * g + 8, :] = top
            lo[part, 8 * g : 8 * g + 8, :] = (band - top.astype(F32)).astype(BF16)
    for at, ref in enumerate((x, h)):
        a = ref[:1024, :]
        b = ref[1024:, :]
        for held, value in ((ev, a + b), (od, a - b)):
            top = value.astype(BF16)
            held[0, :, at * LANES : (at + 1) * LANES] = top
            held[1, :, at * LANES : (at + 1) * LANES] = (value - top.astype(F32)).astype(BF16)
    for b in range(4):
        span = slice(1024 - 256 * b, 2048 - 256 * b)
        sums = []
        for part, held in ((0, ev), (1, od)):
            high = hi[part, :, span]
            low = lo[part, :, span]
            sums.append(
                jnp.dot(high, held[0], preferred_element_type=F32)
                + jnp.dot(high, held[1], preferred_element_type=F32)
                + jnp.dot(low, held[0], preferred_element_type=F32)
            )
        out[256 * b : 256 * b + 256, :] = sums[0] + sums[1]
        out[1024 + 256 * b : 1280 + 256 * b, :] = sums[0] - sums[1]


def pack_kernel(an, ap, xleft, xright):
    pack(an[...], xleft, xright, 0)
    pack(ap[:ROWS_A, :], xleft, xright, ROWS_A // 4)


def score_stage(count, cases, blocks, flags, row_high, row_low, col_high, col_low, d, yh, yl, out, sem, keep, base):
    length = count * WINDOW + 64
    filled = []
    for start, rows, make in blocks:
        filled.append((start, start + rows))
        am, ah, bm, bh = make()
        has_ahead = flags[0] > 0
        has_behind = flags[1] > 0
        pairs = (
            (jnp.where(has_ahead, am, bm), jnp.where(has_ahead, ah, bh)),
            (jnp.where(has_behind, bm, am), jnp.where(has_behind, bh, ah)),
        )
        here = slice(start, start + rows)
        for which, (main, edge) in enumerate(pairs):
            side = slice(which * LANES, (which + 1) * LANES)
            d[here, side] = main
            high, low = split(jnp.concatenate([main, edge], axis=1))
            for tile in range(2):
                part = slice(256 * tile, 256 * tile + 256)
                y = jnp.dot(high, row_high[:, part], preferred_element_type=F32)
                y = y + jnp.dot(low, row_high[:, part], preferred_element_type=F32)
                if tile:
                    y = y + jnp.dot(high, row_low[...], preferred_element_type=F32)
                top, rest = split(y)
                for k in range(2):
                    yh[2 * tile + k, here, side] = top[:, k * LANES : (k + 1) * LANES]
                    yl[2 * tile + k, here, side] = rest[:, k * LANES : (k + 1) * LANES]
    gaps = [(filled[i][1], filled[i + 1][0]) for i in range(len(filled) - 1)]
    for low, high in [(0, filled[0][0])] + gaps + [(filled[-1][1], length)]:
        if low < high:
            for k in range(4):
                yh[k, low:high, :] = jnp.zeros((high - low, 256), BF16)
                yl[k, low:high, :] = jnp.zeros((high - low, 256), BF16)
    copies = []
    for w in range(count):
        case = cases[0] if w == 0 else cases[2] if w == count - 1 else cases[1]
        span = slice(WINDOW * w, WINDOW * w + 256)
        before = d[HALO + WINDOW * w : HALO + WINDOW * (w + 1), :]
        score = None
        for k in range(4):
            after = jnp.dot(col_high[case, k], yh[k, span, :], preferred_element_type=F32)
            after = after + jnp.dot(col_high[case, k], yl[k, span, :], preferred_element_type=F32)
            if k >= 2:
                after = after + jnp.dot(col_low[case, k - 2], yh[k, span, :], preferred_element_type=F32)
            gap = before - after
            score = gap * gap if score is None else score + 2.0**k * (gap * gap)
            before = after
        d[HALO + WINDOW * w : HALO + WINDOW * (w + 1), :LANES] = score[:, :LANES] * score[:, LANES:]
    low, high = keep
    copy = pltpu.make_async_copy(
        d.at[pl.ds(HALO + low, high - low), pl.ds(0, LANES)], out.at[pl.ds(base + low, high - low)], sem
    )
    copy.start()
    copy.wait()


def first_kernel(flags, sa, sb, an, ap, gright, gleft, rh, rl, ch, cl, out, d, yh, yl, sem):
    n = ROWS_A // 4

    def block(q):
        def make():
            here = slice(q * n, q * n + n)
            parts = []
            for which, (own, other) in enumerate(((sa, an), (sb, ap))):
                edge = unpack(gright[which * n : which * n + n, :], gleft[which * n : which * n + n, :], q)
                parts += [own[here, :LANES] - other[here, :], own[here, LANES:] - edge]
            return parts

        return (HALO + q * n, n, make)

    score_stage(
        WINDOWS_A, (0, 1, 1), [block(q) for q in range(4)], flags, rh, rl, ch, cl, d, yh, yl, out, sem, (0, KEEP_A), 0
    )


def second_kernel(flags, sa, sb, an, ap, gright, gleft, bn, bp, rh, rl, ch, cl, _, out, d, yh, yl, sem):
    n = ROWS_A // 4
    half = ROWS_B // 2
    lane = lanes((half, LANES))

    def old():
        parts = []
        for which, (own, other) in enumerate(((sa, an), (sb, ap))):
            last = slice(which * n + n - OLD_B, which * n + n)
            edge = unpack(gright[last, :], gleft[last, :], 3)
            parts += [
                own[START_B:ROWS_A, :LANES] - other[START_B:ROWS_A, :],
                own[START_B:ROWS_A, LANES:] - edge,
            ]
        return parts

    def fresh(q):
        def make():
            here = slice(ROWS_A + q * half, ROWS_A + q * half + half)
            parts = []
            for own, new in ((sa, bn), (sb, bp)):
                both = new[ROWS_B:, :]
                right = pltpu.roll(both, 96, 1) if q else both
                left = both if q else pltpu.roll(both, 32, 1)
                edge = jnp.where(lane < 32, right, jnp.where(lane >= 96, left, 0.0))
                parts += [
                    own[here, :LANES] - new[q * half : q * half + half, :],
                    own[here, LANES:] - edge,
                ]
            return parts

        return (OLD_B + q * half, half, make)

    blocks = [(0, OLD_B, old), fresh(0), fresh(1)]
    base = START_B + HALO
    score_stage(
        WINDOWS_B,
        (1, 1, 2),
        blocks,
        flags,
        rh,
        rl,
        ch,
        cl,
        d,
        yh,
        yl,
        out,
        sem,
        (KEEP_A - base, COLS - base),
        base,
    )


def struct(*shape):
    return jax.ShapeDtypeStruct(shape, F32)


def cost(flops):
    return pl.CostEstimate(flops=flops, bytes_accessed=0, transcendentals=0)


def shards(image, offsets):
    x = image[0]
    position = lax.axis_index("bulk")
    side = lax.axis_index("swath")
    tiles = lax.axis_size("bulk")
    count = lax.axis_size("swath")
    toward = [(i, i + DIE_SPAN) for i in range(tiles - DIE_SPAN)]
    back = [(j, i) for i, j in toward]
    up = [(i, i + 1) for i in range(count - 1)]
    down = [(j, i) for i, j in up]
    flags = jnp.stack([position + DIE_SPAN < tiles, position >= DIE_SPAN, side > 0, side < count - 1]).astype(jnp.int32)
    rh, rl, ch, cl = pl.pallas_call(
        tables_kernel,
        out_shape=(
            jax.ShapeDtypeStruct((256, 512), BF16),
            jax.ShapeDtypeStruct((256, 256), BF16),
            jax.ShapeDtypeStruct((3, 4, WINDOW, 256), BF16),
            jax.ShapeDtypeStruct((3, 2, WINDOW, 256), BF16),
        ),
        in_specs=[SMEM],
        out_specs=(VMEM,) * 4,
        compiler_params=PARAMS,
        cost_estimate=cost(2_000_000_000),
        name="tables",
    )(flags)

    adn, aup, ny, pleft, pright = pl.pallas_call(
        head_kernel,
        out_shape=(
            struct(ROWS_A, LANES),
            struct(ROWS_A + 8, LANES),
            struct(8, LANES),
            struct(COLS // 4, LANES),
            struct(COLS // 4, LANES),
        ),
        in_specs=[SMEM, VMEM],
        out_specs=(VMEM,) * 5,
        compiler_params=PARAMS,
        name="head",
    )(offsets, x)
    an = lax.ppermute(adn, "bulk", back)
    ap = lax.ppermute(aup, "bulk", toward)
    from_right = lax.ppermute(pleft, "swath", down)
    from_left = lax.ppermute(pright, "swath", up)
    packed_b = ROWS_B + ROWS_B // 2
    h, bdn, bup = pl.pallas_call(
        edge_kernel,
        out_shape=(struct(COLS, LANES), struct(packed_b, LANES), struct(packed_b, LANES)),
        in_specs=[SMEM] + [VMEM] * 4,
        out_specs=(VMEM,) * 3,
        compiler_params=PARAMS,
        name="edge",
    )(offsets, x, ny, from_right, from_left)
    bn = lax.ppermute(bdn, "bulk", back)
    bp = lax.ppermute(bup, "bulk", toward)

    def shift(sign, move, spec):
        return pl.pallas_call(
            functools.partial(shift_kernel, sign),
            out_shape=struct(COLS, 2 * LANES),
            in_specs=[spec, VMEM, VMEM],
            out_specs=VMEM,
            scratch_shapes=[
                pltpu.VMEM((2, 256, COLS), BF16),
                pltpu.VMEM((2, 256, COLS), BF16),
                pltpu.VMEM((2, 1024, 256), BF16),
                pltpu.VMEM((2, 1024, 256), BF16),
            ],
            compiler_params=PARAMS,
            cost_estimate=cost(3_000_000_000),
            name="shift" + ("own" if sign > 0 else "back"),
        )(move, x, h)

    sa = shift(1, offsets, SMEM)
    quarter = ROWS_A // 2
    xleft, xright = pl.pallas_call(
        pack_kernel,
        out_shape=(struct(quarter, LANES), struct(quarter, LANES)),
        in_specs=[VMEM] * 2,
        out_specs=(VMEM,) * 2,
        compiler_params=PARAMS,
        name="pack",
    )(an, ap)
    gright = lax.ppermute(xleft, "swath", down)
    gleft = lax.ppermute(xright, "swath", up)
    sb = shift(-1, ap, VMEM)

    def scratch(count):
        length = count * WINDOW + 64
        return [
            pltpu.VMEM((length, 256), F32),
            pltpu.VMEM((4, length, 256), BF16),
            pltpu.VMEM((4, length, 256), BF16),
            pltpu.SemaphoreType.DMA,
        ]

    first = pl.pallas_call(
        first_kernel,
        out_shape=struct(COLS, LANES),
        in_specs=[SMEM] + [VMEM] * 10,
        out_specs=ANY,
        scratch_shapes=scratch(WINDOWS_A),
        compiler_params=PARAMS,
        cost_estimate=cost(3_000_000_000),
        name="first",
    )(flags, sa, sb, an, ap, gright, gleft, rh, rl, ch, cl)
    whole = pl.pallas_call(
        second_kernel,
        out_shape=struct(COLS, LANES),
        in_specs=[SMEM] + [VMEM] * 12 + [ANY],
        out_specs=ANY,
        scratch_shapes=scratch(WINDOWS_B),
        input_output_aliases={13: 0},
        compiler_params=PARAMS,
        name="second",
    )(flags, sa, sb, an, ap, gright, gleft, bn, bp, rh, rl, ch, cl, first)
    return whole[None]


def solution(mesh):
    return jax.shard_map(
        shards,
        mesh=mesh,
        in_specs=(P("bulk", None, "swath"), P("bulk")),
        out_specs=P("bulk", None, "swath"),
        check_vma=False,
    )
```

```python
import functools
import math

import jax
import jax.numpy as jnp
from jax import lax
from jax.experimental import pallas as pl
from jax.experimental.pallas import tpu as pltpu
from jax.sharding import PartitionSpec as P

DIE_SPAN = 4
COLS = 2048
LANES = 128
HALO = 32
ROWS_A = 1152
ROWS_B = COLS - ROWS_A
KEEP_A = ROWS_A - 32
WINDOW = 192
WINDOWS_A = -(-KEEP_A // WINDOW)
WINDOWS_B = -(-(COLS - KEEP_A) // WINDOW)
START_B = COLS - WINDOWS_B * WINDOW - HALO
OLD_B = ROWS_A - START_B

F32 = jnp.float32
BF16 = jnp.bfloat16
VMEM = pl.BlockSpec(memory_space=pltpu.VMEM)
SMEM = pl.BlockSpec(memory_space=pltpu.SMEM)
ANY = pl.BlockSpec(memory_space=pl.ANY)
PARAMS = pltpu.CompilerParams(vmem_limit_bytes=40 << 20)


def split(value):
    high = value.astype(BF16)
    return high, (value - high.astype(F32)).astype(BF16)


def tables_kernel(flags, row_high, row_low, col_high, col_low):
    shape = (256, 256)
    down = lax.broadcasted_iota(jnp.int32, shape, 0)
    across = lax.broadcasted_iota(jnp.int32, shape, 1)
    apart = (down - across) & 255
    apart = jnp.minimum(apart, 256 - apart)
    blurs = []
    for octave in range(4):
        reach = 2**octave
        weight = jnp.where(apart == 0, 6.0, jnp.where(apart == reach, 4.0, jnp.where(apart == 2 * reach, 1.0, 0.0)))
        blurs.append(weight.astype(BF16))
    inside = (across < LANES).astype(jnp.int32)
    inside = inside + ((across >= LANES) & (across < LANES + HALO)).astype(jnp.int32) * flags[3]
    inside = (inside + (across >= 256 - HALO).astype(jnp.int32) * flags[2]).astype(F32)
    total = jnp.where(down == across, inside, 0.0)
    for octave in range(4):
        high, low = split(total)
        total = inside * (
            jnp.dot(high, blurs[octave], preferred_element_type=F32)
            + jnp.dot(low, blurs[octave], preferred_element_type=F32)
        )
        high, low = split(total[:, :LANES] * 256.0 ** -(octave + 1))
        row_high[:, octave * LANES : (octave + 1) * LANES] = high
        if octave >= 2:
            row_low[:, (octave - 2) * LANES : (octave - 1) * LANES] = low
    for case, inside in enumerate((down >= HALO, down >= 0, down < 256 - HALO)):
        inside = inside.astype(F32)
        total = jnp.where(down == across, inside, 0.0)
        for octave in range(4):
            high, low = split(total)
            total = inside * (
                jnp.dot(blurs[octave], high, preferred_element_type=F32)
                + jnp.dot(blurs[octave], low, preferred_element_type=F32)
            )
            high, low = split(total[HALO : 256 - HALO])
            col_high[case, octave] = high
            if octave >= 2:
                col_low[case, octave - 2] = low


def lanes(shape):
    return lax.broadcasted_iota(jnp.int32, shape, 1)


def signs(shape):
    return (1 - 2 * (lax.broadcasted_iota(jnp.int32, shape, 0) % 2)).astype(F32)


def sine(x):
    y = x * x
    total = jnp.full_like(x, 1 / math.factorial(13))
    for power in (11, 9, 7, 5, 3, 1):
        total = total * y + (-1) ** ((power - 1) // 2) / math.factorial(power)
    return total * x


def cosine(x):
    y = x * x
    total = jnp.full_like(x, -1 / math.factorial(14))
    for power in (12, 10, 8, 6, 4, 2, 0):
        total = total * y + (-1) ** (power // 2) / math.factorial(power)
    return total


def turned_sine(moves):
    turns = jnp.floor(moves * (1 / 64) + 0.5)
    parity = turns - 2 * jnp.floor(turns * 0.5)
    return (1 - 2 * parity) * sine((moves - 64 * turns) * (math.pi / 64))


def nyquist(v):
    folded = v.reshape(COLS // 8, 8, LANES).sum(axis=0)
    return jnp.sum(folded * signs((8, LANES)), axis=0, keepdims=True) * (1 / COLS)


def pack(v, out_left, out_right, at):
    n = v.shape[0] // 4
    lane = lanes((n, LANES))
    left = right = None
    for q in range(4):
        piece = v[q * n : (q + 1) * n]
        here = (lane >= 32 * q) & (lane < 32 * q + 32)
        to_left = pltpu.roll(piece, 32 * q, 1) if q else piece
        to_right = pltpu.roll(piece, (32 * q + 32) % 128, 1) if q < 3 else piece
        left = to_left if left is None else jnp.where(here, to_left, left)
        right = to_right if right is None else jnp.where(here, to_right, right)
    out_left[at : at + n, :] = left
    out_right[at : at + n, :] = right


def unpack(from_right, from_left, q):
    lane = lanes(from_right.shape)
    right = pltpu.roll(from_right, (128 - 32 * q) % 128, 1) if q else from_right
    left = pltpu.roll(from_left, (96 - 32 * q) % 128, 1) if q < 3 else from_left
    return jnp.where(lane < HALO, right, jnp.where(lane >= LANES - HALO, left, 0.0))


def head_kernel(move, x, adn, aup, ny, pleft, pright):
    v = x[...]
    own = move[0].astype(F32)
    tone = nyquist(v)
    ny[...] = jnp.broadcast_to(tone, (8, LANES))
    wave = turned_sine(jnp.full((8, LANES), own, F32))
    swing = (wave * wave * jnp.broadcast_to(tone, (8, LANES)) * signs((8, LANES)))[None]
    adn[...] = v[:ROWS_A]
    first = v[:ROWS_A].reshape(ROWS_A // 8, 8, LANES) - swing
    aup[:ROWS_A, :] = first.reshape(ROWS_A, LANES)
    aup[ROWS_A:, :] = jnp.full((8, LANES), own, F32)
    pack(v, pleft, pright, 0)


def edge_kernel(move, x, ny, from_right, from_left, h, bdn, bup):
    n = COLS // 4
    for q in range(4):
        h[q * n : (q + 1) * n, :] = unpack(from_right[...], from_left[...], q)
    own = move[0].astype(F32)
    wave = turned_sine(jnp.full((8, LANES), own, F32))
    gain = wave * wave * signs((8, LANES))
    swing = (gain * ny[...])[None]
    hswing = (gain * jnp.broadcast_to(nyquist(h[...]), (8, LANES)))[None]
    half = ROWS_B // 2
    lane = lanes((half, LANES))

    def put(main, edge, out):
        out[:ROWS_B, :] = main
        one, two = edge[:half], edge[half:]
        out[ROWS_B:, :] = jnp.where(
            lane < 32,
            one,
            jnp.where(lane < 64, pltpu.roll(two, 32, 1), jnp.where(lane < 96, pltpu.roll(one, 96, 1), two)),
        )

    main = x[ROWS_A:, :]
    edge = h[ROWS_A:, :]
    put(main, edge, bdn)
    shape = (ROWS_B // 8, 8, LANES)
    put(
        (main.reshape(shape) - swing).reshape(ROWS_B, LANES),
        (edge.reshape(shape) - hswing).reshape(ROWS_B, LANES),
        bup,
    )


def shift_kernel(sign, move, x, h, out, hi, lo, ev, od):
    if sign > 0:
        moves = jnp.full((8, COLS), move[0].astype(F32), F32)
    else:
        moves = -jnp.concatenate([move[ROWS_A:, :]] * (COLS // LANES), axis=1)
    place = lax.broadcasted_iota(jnp.int32, (8, COLS), 1)
    delay = (1024 - place).astype(F32)
    steps = 64 * delay - moves
    turns = jnp.floor(steps * (1 / 65536) + 0.5)
    rest = steps - 65536 * turns
    flip = 1 - 2 * (turns - 2 * jnp.floor(turns * 0.5))
    theta = rest * (math.pi / 65536)
    hit = rest == 0.0
    parity = (1 - 2 * (place % 2)).astype(F32)
    base = parity * turned_sine(moves) * (-0.5 / 1024) / jnp.where(hit, 1.0, sine(theta))
    even = jnp.where(hit, 0.5, base * cosine(theta))
    odd = flip * jnp.where(hit, 0.5, base)
    for part, row in enumerate((even, odd)):
        slope = pltpu.roll(row, 0, 1, stride=1, stride_axis=0)
        for g in range(32):
            band = pltpu.roll(slope, 8 * g, 1) if g else slope
            top = band.astype(BF16)
            hi[part, 8 * g : 8 * g + 8, :] = top
            lo[part, 8 * g : 8 * g + 8, :] = (band - top.astype(F32)).astype(BF16)
    for at, ref in enumerate((x, h)):
        a = ref[:1024, :]
        b = ref[1024:, :]
        for held, value in ((ev, a + b), (od, a - b)):
            top = value.astype(BF16)
            held[0, :, at * LANES : (at + 1) * LANES] = top
            held[1, :, at * LANES : (at + 1) * LANES] = (value - top.astype(F32)).astype(BF16)
    for b in range(4):
        span = slice(1024 - 256 * b, 2048 - 256 * b)
        sums = []
        for part, held in ((0, ev), (1, od)):
            high = hi[part, :, span]
            low = lo[part, :, span]
            sums.append(
                jnp.dot(high, held[0], preferred_element_type=F32)
                + jnp.dot(high, held[1], preferred_element_type=F32)
                + jnp.dot(low, held[0], preferred_element_type=F32)
            )
        out[256 * b : 256 * b + 256, :] = sums[0] + sums[1]
        out[1024 + 256 * b : 1280 + 256 * b, :] = sums[0] - sums[1]


def pack_kernel(an, ap, xleft, xright):
    pack(an[...], xleft, xright, 0)
    pack(ap[:ROWS_A, :], xleft, xright, ROWS_A // 4)


def score_stage(count, cases, blocks, flags, row_high, row_low, col_high, col_low, d, yh, yl, emit):
    length = count * WINDOW + 64
    filled = []
    for start, rows, make in blocks:
        filled.append((start, start + rows))
        am, ah, bm, bh = make()
        has_ahead = flags[0] > 0
        has_behind = flags[1] > 0
        pairs = (
            (jnp.where(has_ahead, am, bm), jnp.where(has_ahead, ah, bh)),
            (jnp.where(has_behind, bm, am), jnp.where(has_behind, bh, ah)),
        )
        here = slice(start, start + rows)
        for which, (main, edge) in enumerate(pairs):
            side = slice(which * LANES, (which + 1) * LANES)
            d[here, side] = main
            high, low = split(jnp.concatenate([main, edge], axis=1))
            for tile in range(2):
                part = slice(256 * tile, 256 * tile + 256)
                y = jnp.dot(high, row_high[:, part], preferred_element_type=F32)
                y = y + jnp.dot(low, row_high[:, part], preferred_element_type=F32)
                if tile:
                    y = y + jnp.dot(high, row_low[...], preferred_element_type=F32)
                top, rest = split(y)
                for k in range(2):
                    yh[2 * tile + k, here, side] = top[:, k * LANES : (k + 1) * LANES]
                    yl[2 * tile + k, here, side] = rest[:, k * LANES : (k + 1) * LANES]
    gaps = [(filled[i][1], filled[i + 1][0]) for i in range(len(filled) - 1)]
    for low, high in [(0, filled[0][0])] + gaps + [(filled[-1][1], length)]:
        if low < high:
            for k in range(4):
                yh[k, low:high, :] = jnp.zeros((high - low, 256), BF16)
                yl[k, low:high, :] = jnp.zeros((high - low, 256), BF16)
    for w in range(count):
        case = cases[0] if w == 0 else cases[2] if w == count - 1 else cases[1]
        span = slice(WINDOW * w, WINDOW * w + 256)
        before = d[HALO + WINDOW * w : HALO + WINDOW * (w + 1), :]
        score = None
        for k in range(4):
            after = jnp.dot(col_high[case, k], yh[k, span, :], preferred_element_type=F32)
            after = after + jnp.dot(col_high[case, k], yl[k, span, :], preferred_element_type=F32)
            if k >= 2:
                after = after + jnp.dot(col_low[case, k - 2], yh[k, span, :], preferred_element_type=F32)
            gap = before - after
            score = gap * gap if score is None else score + 2.0**k * (gap * gap)
            before = after
        emit(w, score[:, :LANES] * score[:, LANES:])


def first_kernel(flags, sa, sb, an, ap, gright, gleft, rh, rl, ch, cl, out, d, yh, yl):
    n = ROWS_A // 4

    def block(q):
        def make():
            here = slice(q * n, q * n + n)
            parts = []
            for which, (own, other) in enumerate(((sa, an), (sb, ap))):
                edge = unpack(gright[which * n : which * n + n, :], gleft[which * n : which * n + n, :], q)
                parts += [own[here, :LANES] - other[here, :], own[here, LANES:] - edge]
            return parts

        return (HALO + q * n, n, make)

    def emit(w, value):
        out[WINDOW * w : WINDOW * (w + 1), :] = value

    score_stage(WINDOWS_A, (0, 1, 1), [block(q) for q in range(4)], flags, rh, rl, ch, cl, d, yh, yl, emit)


def second_kernel(flags, sa, sb, an, ap, gright, gleft, bn, bp, rh, rl, ch, cl, early, out, d, yh, yl, held, sem):
    base = START_B + HALO
    copies = [pltpu.make_async_copy(early.at[pl.ds(0, KEEP_A)], out.at[pl.ds(0, KEEP_A)], sem.at[WINDOWS_B])]
    copies[0].start()
    n = ROWS_A // 4
    half = ROWS_B // 2
    lane = lanes((half, LANES))

    def old():
        parts = []
        for which, (own, other) in enumerate(((sa, an), (sb, ap))):
            last = slice(which * n + n - OLD_B, which * n + n)
            edge = unpack(gright[last, :], gleft[last, :], 3)
            parts += [
                own[START_B:ROWS_A, :LANES] - other[START_B:ROWS_A, :],
                own[START_B:ROWS_A, LANES:] - edge,
            ]
        return parts

    def fresh(q):
        def make():
            here = slice(ROWS_A + q * half, ROWS_A + q * half + half)
            parts = []
            for own, new in ((sa, bn), (sb, bp)):
                both = new[ROWS_B:, :]
                right = pltpu.roll(both, 96, 1) if q else both
                left = both if q else pltpu.roll(both, 32, 1)
                edge = jnp.where(lane < 32, right, jnp.where(lane >= 96, left, 0.0))
                parts += [
                    own[here, :LANES] - new[q * half : q * half + half, :],
                    own[here, LANES:] - edge,
                ]
            return parts

        return (OLD_B + q * half, half, make)

    blocks = [(0, OLD_B, old), fresh(0), fresh(1)]

    def emit(w, value):
        held[WINDOW * w : WINDOW * (w + 1), :] = value
        low = max(WINDOW * w, KEEP_A - base)
        count = WINDOW * (w + 1) - low
        copy = pltpu.make_async_copy(held.at[pl.ds(low, count)], out.at[pl.ds(base + low, count)], sem.at[w])
        copy.start()
        copies.append(copy)

    score_stage(WINDOWS_B, (1, 1, 2), blocks, flags, rh, rl, ch, cl, d, yh, yl, emit)
    for copy in copies:
        copy.wait()


def struct(*shape):
    return jax.ShapeDtypeStruct(shape, F32)


def cost(flops):
    return pl.CostEstimate(flops=flops, bytes_accessed=0, transcendentals=0)


def shards(image, offsets):
    x = image[0]
    position = lax.axis_index("bulk")
    side = lax.axis_index("swath")
    tiles = lax.axis_size("bulk")
    count = lax.axis_size("swath")
    toward = [(i, i + DIE_SPAN) for i in range(tiles - DIE_SPAN)]
    back = [(j, i) for i, j in toward]
    up = [(i, i + 1) for i in range(count - 1)]
    down = [(j, i) for i, j in up]
    flags = jnp.stack([position + DIE_SPAN < tiles, position >= DIE_SPAN, side > 0, side < count - 1]).astype(jnp.int32)
    rh, rl, ch, cl = pl.pallas_call(
        tables_kernel,
        out_shape=(
            jax.ShapeDtypeStruct((256, 512), BF16),
            jax.ShapeDtypeStruct((256, 256), BF16),
            jax.ShapeDtypeStruct((3, 4, WINDOW, 256), BF16),
            jax.ShapeDtypeStruct((3, 2, WINDOW, 256), BF16),
        ),
        in_specs=[SMEM],
        out_specs=(VMEM,) * 4,
        compiler_params=PARAMS,
        cost_estimate=cost(2_000_000_000),
        name="tables",
    )(flags)

    adn, aup, ny, pleft, pright = pl.pallas_call(
        head_kernel,
        out_shape=(
            struct(ROWS_A, LANES),
            struct(ROWS_A + 8, LANES),
            struct(8, LANES),
            struct(COLS // 4, LANES),
            struct(COLS // 4, LANES),
        ),
        in_specs=[SMEM, VMEM],
        out_specs=(VMEM,) * 5,
        compiler_params=PARAMS,
        name="head",
    )(offsets, x)
    an = lax.ppermute(adn, "bulk", back)
    ap = lax.ppermute(aup, "bulk", toward)
    from_right = lax.ppermute(pleft, "swath", down)
    from_left = lax.ppermute(pright, "swath", up)
    packed_b = ROWS_B + ROWS_B // 2
    h, bdn, bup = pl.pallas_call(
        edge_kernel,
        out_shape=(struct(COLS, LANES), struct(packed_b, LANES), struct(packed_b, LANES)),
        in_specs=[SMEM] + [VMEM] * 4,
        out_specs=(VMEM,) * 3,
        compiler_params=PARAMS,
        name="edge",
    )(offsets, x, ny, from_right, from_left)

    def shift(sign, move, spec):
        return pl.pallas_call(
            functools.partial(shift_kernel, sign),
            out_shape=struct(COLS, 2 * LANES),
            in_specs=[spec, VMEM, VMEM],
            out_specs=VMEM,
            scratch_shapes=[
                pltpu.VMEM((2, 256, COLS), BF16),
                pltpu.VMEM((2, 256, COLS), BF16),
                pltpu.VMEM((2, 1024, 256), BF16),
                pltpu.VMEM((2, 1024, 256), BF16),
            ],
            compiler_params=PARAMS,
            cost_estimate=cost(3_000_000_000),
            name="shift" + ("own" if sign > 0 else "back"),
        )(move, x, h)

    sa = shift(1, offsets, SMEM)
    sa, bdn, bup = lax.optimization_barrier((sa, bdn, bup))
    bn = lax.ppermute(bdn, "bulk", back)
    bp = lax.ppermute(bup, "bulk", toward)
    an, ap, sa = lax.optimization_barrier((an, ap, sa))
    quarter = ROWS_A // 2
    xleft, xright = pl.pallas_call(
        pack_kernel,
        out_shape=(struct(quarter, LANES), struct(quarter, LANES)),
        in_specs=[VMEM] * 2,
        out_specs=(VMEM,) * 2,
        compiler_params=PARAMS,
        name="pack",
    )(an, ap)
    gright = lax.ppermute(xleft, "swath", down)
    gleft = lax.ppermute(xright, "swath", up)
    sb = shift(-1, ap, VMEM)

    def scratch(count):
        length = count * WINDOW + 64
        return [
            pltpu.VMEM((length, 256), F32),
            pltpu.VMEM((4, length, 256), BF16),
            pltpu.VMEM((4, length, 256), BF16),
        ]

    first = pl.pallas_call(
        first_kernel,
        out_shape=struct(WINDOWS_A * WINDOW, LANES),
        in_specs=[SMEM] + [VMEM] * 10,
        out_specs=VMEM,
        scratch_shapes=scratch(WINDOWS_A),
        compiler_params=PARAMS,
        cost_estimate=cost(3_000_000_000),
        name="first",
    )(flags, sa, sb, an, ap, gright, gleft, rh, rl, ch, cl)
    whole = pl.pallas_call(
        second_kernel,
        out_shape=struct(COLS, LANES),
        in_specs=[SMEM] + [VMEM] * 13,
        out_specs=ANY,
        scratch_shapes=scratch(WINDOWS_B)
        + [pltpu.VMEM((WINDOWS_B * WINDOW, LANES), F32), pltpu.SemaphoreType.DMA((WINDOWS_B + 1,))],
        compiler_params=PARAMS,
        name="second",
    )(flags, sa, sb, an, ap, gright, gleft, bn, bp, rh, rl, ch, cl, first)
    return whole[None]


def solution(mesh):
    return jax.shard_map(
        shards,
        mesh=mesh,
        in_specs=(P("bulk", None, "swath"), P("bulk")),
        out_specs=P("bulk", None, "swath"),
        check_vma=False,
    )
```
